32 devices in a mesh: grp: 2 (over y), img: 4 (over z), dim: 2 (over x), qry: 2 (over core).
Axes of the slice: x: 2, y: 2, z: 4, core: 2. Of those that a mesh axis runs over, the one named last changes fastest.
Arguments:
- caption_vectors: bfloat16 [1024, 1152], P(('grp', 'img', 'qry'), 'dim'), parts along dimension 0, may hold values from -12 to 12
- logit_multiplier: float32 [1024], P(('grp', 'img', 'qry')), parts along dimension 0, may hold values from 0.5 to 8
- picture_vectors: bfloat16 [8192, 1152], P(('grp', 'img'), 'dim'), parts along dimension 0, may hold values from -6 to 6
Outputs:
- lse: float32 [1024], P(('grp', 'img', 'qry')), parts along dimension 0
- top_scores: float32 [1024, 10], P(('grp', 'img', 'qry')), parts along dimension 0
The draws below stay inside these ranges and needn't reach their ends.
There are 2 independent parts, one for each index of `grp`. The reference program is written for one: setup_inputs(seed, part) draws one part's arguments, and reference() takes and returns one part's arrays. A program takes and returns all parts, laid end to end along the dimension named above; each array names one. Nothing has to cross between parts.
All inputs are finite; a program needn't handle non-finite values.
Results may differ from the reference program's by a relative error of at most 0.00073.
Values may be sent and summed in bfloat16 or wider, within the bound.
A program may use at most 64 MiB of HBM per device.

```python
import math
import jax
import jax.numpy as jnp
from jax import lax

FEATURE_SPAN = 1152
K = 10
IMAGES_PER_SHARD = 1024
PROMPT_COUNT = 512
NIMG = 4096
N_IMG = 4


def image_table(key):
    run_count = NIMG // 16
    run_base = jax.random.normal(jax.random.fold_in(key, 11), (run_count, FEATURE_SPAN), jnp.float32)
    spread = jnp.repeat(run_base, 16, axis=0)
    noise = jax.random.normal(jax.random.fold_in(key, 13), (NIMG, FEATURE_SPAN), jnp.float32)
    return jnp.clip(0.95 * spread + 0.3 * noise, -6.0, 6.0)


def draw_picture_vectors(key, part):
    return image_table(key).astype(jnp.bfloat16)


def draw_caption_vectors(key, part):
    base = jnp.clip(jax.random.normal(jax.random.fold_in(key, 23), (PROMPT_COUNT, FEATURE_SPAN), jnp.float32), -6.0, 6.0)
    table = image_table(key)
    count = PROMPT_COUNT // 32
    picks = jax.random.randint(jax.random.fold_in(key, 41), (count,), 0, NIMG)
    places = jnp.arange(count) * 32 + 8
    mixed = 0.4 * table[picks] + 0.6 * base[places]
    mixed = jnp.clip(mixed, -12.0, 12.0)
    base = base.at[places].set(mixed)
    return base.astype(jnp.bfloat16)


def block_scale(key, extent, cuts, least, top_value):
    def one(position, parts):
        heights = jax.random.uniform(jax.random.fold_in(jax.random.fold_in(key, 6), position), (parts,), jnp.float32, least / len(cuts), top_value / len(cuts))
        return jnp.repeat(jnp.exp(heights), extent[position] // parts).reshape((-1,) + (1,) * (len(extent) - position - 1))

    level = one(*cuts[0])
    for cut in cuts[1:]:
        level = level * one(*cut)
    return level


def setup_inputs(seed: int = 0, part: int = 0) -> dict:
    streams_of = jax.random.split(jax.random.key(seed), 4)
    part_keys = jax.random.split(jax.random.fold_in(streams_of[3], part), 4)
    caption_vectors = draw_caption_vectors(jax.random.fold_in(jax.random.fold_in(streams_of[3], part), 71), part)
    logit_multiplier = jnp.clip(jnp.exp(math.log(8.0) - 2.7725887 * jax.random.uniform(part_keys[1], (PROMPT_COUNT,), jnp.float32) ** block_scale(part_keys[1], (PROMPT_COUNT,), ((0, 8),), -0.2, 0.2)), 0.5, 8.0)
    picture_vectors = draw_picture_vectors(jax.random.fold_in(jax.random.fold_in(streams_of[3], part), 71), part)
    return {"caption_vectors": caption_vectors, "logit_multiplier": logit_multiplier, "picture_vectors": picture_vectors}


def reference(caption_vectors, logit_multiplier, picture_vectors):
    sharpened_logits = (logit_multiplier[:, None] * caption_vectors.astype(jnp.float32) * (FEATURE_SPAN ** -0.5)).astype(jnp.bfloat16)
    picture_tiles = picture_vectors.reshape(N_IMG, IMAGES_PER_SHARD, FEATURE_SPAN)

    def step(carry, block):
        best, total = carry
        scores = jnp.dot(sharpened_logits, block.T, preferred_element_type=jnp.float32)
        block_top = lax.top_k(scores, K)[0]
        tile_number = jnp.sum(jnp.exp(scores - block_top[:, :1]), axis=1)
        peak = jnp.maximum(best[:, 0], block_top[:, 0])
        total = total * jnp.exp(best[:, 0] - peak) + tile_number * jnp.exp(block_top[:, 0] - peak)
        best = lax.top_k(jnp.concatenate([best, block_top], axis=1), K)[0]
        return (best, total), None

    start = (jnp.full((PROMPT_COUNT, K), -1e30, jnp.float32), jnp.zeros((PROMPT_COUNT,), jnp.float32))
    (best, total), unused = lax.scan(step, start, picture_tiles)
    return best[:, 0] + jnp.log(total), best
```

```python
import functools

import jax
import jax.numpy as jnp
from jax import lax
from jax.experimental import pallas as pl
from jax.experimental.pallas import tpu as pltpu
from jax.sharding import PartitionSpec as P

K = 10
LIST = 16
PAY = 16
LANES = 128
SUB = 8
SPAN = 83.0
TAIL = 16
MESH = pl.DeviceIdType.MESH


def xor_index(a, b, n):
    out, bit = 0, 1
    while bit < n:
        p, q = lax.rem(a // bit, 2), lax.rem(b // bit, 2)
        out = out + bit * (p + q - 2 * p * q)
        bit *= 2
    return out


def exchange(v, i, j):
    hi, lo = jnp.maximum(v[i], v[j]), jnp.minimum(v[i], v[j])
    v[i], v[j] = hi, lo


def sort_desc(v):
    v = list(v)
    n = len(v)
    p = 1
    while p < n:
        k = p
        while k >= 1:
            for j in range(k % p, n - k, 2 * k):
                for i in range(min(k, n - j - k)):
                    if (i + j) // (2 * p) == (i + j + k) // (2 * p):
                        exchange(v, i + j, i + j + k)
            k //= 2
        p *= 2
    return v


def merge_desc(a, b):
    v = [jnp.maximum(a[i], b[LIST - 1 - i]) for i in range(LIST)]
    step = LIST // 2
    while step:
        for i in range(LIST):
            if not i & step:
                exchange(v, i, i + step)
        step //= 2
    return v


def merge_all(lists):
    while len(lists) > 1:
        merged = [merge_desc(lists[i], lists[i + 1]) for i in range(0, len(lists) - 1, 2)]
        lists = merged + lists[len(lists) - len(lists) % 2:]
    return lists[0]


def fold_sublanes(v):
    for shift in (4, 2, 1):
        v = merge_desc(v, [pltpu.roll(x, shift, 0) for x in v])
    return v


def for_each(lo, hi, body):
    if hi - lo <= 4:
        for k in range(lo, hi):
            body(k)
    else:
        lax.fori_loop(lo, hi, lambda k, c: (body(k), c)[1], 0)


def kernel(nd, nz, scale, cap_hbm, mult_hbm, img_hbm, res_ref,
           cap_ref, mult_ref, in_sem,
           img_in, img, qbuf, own, sent, got, pay, fin,
           img_sem, q_send, q_recv, p_send, p_recv, f_send, f_recv):
    x, z = lax.axis_index("dim"), lax.axis_index("img")
    rows = cap_ref.shape[0]
    half = own.shape[1]
    nsrc = nd * nz

    def at_x(j):
        return lax.rem(x + j, nd)

    def at_z(k):
        return xor_index(z, k, nz)

    def columns(j):
        return pl.ds(pl.multiple_of(at_x(j) * (2 * half), 2 * half), 2 * half)

    def load(j):
        return pltpu.make_async_copy(img_hbm.at[:, columns(j)], img_in.at[j], img_sem.at[j])

    cap_load = pltpu.make_async_copy(cap_hbm, cap_ref, in_sem.at[0])
    mult_load = pltpu.make_async_copy(mult_hbm, mult_ref, in_sem.at[1])
    cap_load.start()
    mult_load.start()
    for j in list(range(1, nd)) + [0]:
        load(j).start()

    barrier = pltpu.get_barrier_semaphore()

    def greet(n):
        k, j = n // nd, lax.rem(n, nd)
        pl.semaphore_signal(barrier, inc=1, device_id={"dim": at_x(j), "img": at_z(k)}, device_id_type=MESH)

    for_each(1, nsrc, greet)

    mult_load.wait()
    cap_load.wait()
    r = lax.broadcasted_iota(jnp.int32, (rows, rows), 0)
    c = lax.broadcasted_iota(jnp.int32, (rows, rows), 1)
    mult = jnp.sum(jnp.where(r == c, jnp.broadcast_to(mult_ref[...], (rows, rows)), 0.0), axis=1, keepdims=True)
    width = cap_ref.shape[1]
    pad = (LANES // 2, width)

    def clear(k):
        qbuf[k, : LANES // 2] = jnp.zeros(pad, jnp.bfloat16)
        qbuf[k, LANES:] = jnp.zeros(pad, jnp.bfloat16)

    for_each(0, nz, clear)
    qbuf[0, LANES // 2 : LANES] = (mult * cap_ref[...].astype(jnp.float32) * scale).astype(jnp.bfloat16)
    pl.semaphore_wait(barrier, nsrc - 1)

    def q_copy(k):
        middle = pl.ds(LANES // 2, LANES // 2)
        return pltpu.make_async_remote_copy(
            src_ref=qbuf.at[0, middle], dst_ref=qbuf.at[k, middle],
            send_sem=q_send.at[k], recv_sem=q_recv.at[k],
            device_id={"dim": x, "img": at_z(k)}, device_id_type=MESH)

    def p_copy(k, j):
        return pltpu.make_async_remote_copy(
            src_ref=sent.at[k, j - 1], dst_ref=got.at[k, j - 1],
            send_sem=p_send.at[k, j - 1], recv_sem=p_recv.at[k, j - 1],
            device_id={"dim": at_x(j), "img": z}, device_id_type=MESH)

    def f_copy(k, j):
        return pltpu.make_async_remote_copy(
            src_ref=pay.at[k], dst_ref=fin.at[k * nd + j],
            send_sem=f_send.at[k, j], recv_sem=f_recv.at[k, j],
            device_id={"dim": at_x(j), "img": at_z(k)}, device_id_type=MESH)

    for_each(1, nz, lambda k: q_copy(k).start())

    nt = (((1,), (1,)), ((), ()))

    def partial(k, j):
        first = lax.dot_general(img[j, :half], qbuf[k, LANES // 2 :], nt, preferred_element_type=jnp.float32)
        return first + lax.dot_general(img[j, half:], qbuf[k, :LANES], nt, preferred_element_type=jnp.float32)

    def encode(part, to):
        bound = jnp.maximum(jnp.max(jnp.abs(part), axis=0, keepdims=True) * 1.01, 1e-30).astype(jnp.bfloat16)
        rate = SPAN / bound.astype(jnp.float32)
        to[:half] = jnp.exp(part * rate).astype(jnp.bfloat16)
        to[half:] = jnp.broadcast_to(bound, (TAIL, LANES))

    def turn(j):
        load(j).wait()
        img[j] = img_in[j].T

    def multiply(k, opening=False):
        for j in range(1, nd):
            if opening:
                turn(j)
            encode(partial(k, j), sent.at[k, j - 1])
            p_copy(k, j).start()
        if opening:
            turn(0)
        own[k] = partial(k, 0)

    def select(k):
        for j in range(1, nd):
            p_copy(k, j).wait_recv()
        unit = [got[k, j - 1, half:].astype(jnp.float32)[:SUB] * (1.0 / SPAN) for j in range(1, nd)]
        tiles = []
        for t in range(0, half, 2 * SUB):
            s = own[k, t : t + 2 * SUB]
            code = [jnp.log(got[k, j - 1, t : t + 2 * SUB].astype(jnp.float32)) for j in range(1, nd)]
            for h in range(0, 2 * SUB, SUB):
                v = s[h : h + SUB]
                for j in range(1, nd):
                    v = v + code[j - 1][h : h + SUB] * unit[j - 1]
                tiles.append(v)
        low = jnp.full((SUB, LANES), -jnp.inf, jnp.float32)
        padded = tiles + [low] * (-len(tiles) % LIST)
        lists = [sort_desc(padded[i : i + LIST]) for i in range(0, len(padded), LIST)]
        best = merge_all(lists)
        best = merge_desc(best, [pltpu.roll(v, LANES // 2, 1) for v in best])
        best = fold_sublanes(best)
        sums = [jnp.exp(s - best[0]) for s in tiles]
        while len(sums) > 1:
            sums = [a + b for a, b in zip(sums[::2], sums[1::2])]
        total = jnp.sum(sums[0], axis=0, keepdims=True)
        total = total + pltpu.roll(total, LANES // 2, 1)
        for i in range(K):
            pay[k, i : i + 1] = best[i][:1]
        pay[k, K : K + 1] = total

    def deliver(k, first):
        for j in range(first, nd):
            f_copy(k, j).start()

    def later(k):
        q_copy(k).wait_recv()
        multiply(k)
        if isinstance(k, int) and k == 1:
            finish_first()
        else:
            select(k - 1)
            deliver(k - 1, 0)

    def finish_first():
        select(0)
        fin[0] = pay[0]
        deliver(0, 1)

    pay[...] = jnp.zeros(pay.shape, jnp.float32)
    multiply(0, True)
    if nz > 1:
        later(1)
        for_each(2, nz, later)
        select(nz - 1)
        deliver(nz - 1, 0)
    else:
        finish_first()

    def arrived(n):
        f_copy(n // nd, lax.rem(n, nd)).wait_recv()

    for_each(1, nsrc, arrived)

    low = jnp.full((SUB, LANES), -jnp.inf, jnp.float32)
    lists = []
    for g in range(0, nsrc, SUB):
        lists.append([fin[g : g + SUB, i] for i in range(K)] + [low] * (LIST - K))
    best = fold_sublanes(merge_all([list(v) for v in lists]))
    total = 0.0
    for g in range(0, nsrc, SUB):
        total = total + fin[g : g + SUB, K] * jnp.exp(fin[g : g + SUB, 0] - best[0])
    lse = best[0][:1] + jnp.log(jnp.sum(total, axis=0, keepdims=True))
    res_ref[...] = jnp.concatenate([v[:1] for v in best[:K]] + [lse] + [v[:1] for v in best[K + 1 :]], axis=0)

    for_each(1, nz, lambda k: q_copy(k).wait_send())

    def drained(k):
        for j in range(1, nd):
            p_copy(k, j).wait_send()

    for_each(0, nz, drained)

    def gone(n):
        f_copy(n // nd, lax.rem(n, nd)).wait_send()

    for_each(1, nsrc, gone)


def split_kernel(res_ref, lse_ref, top_ref):
    rows = lse_ref.shape[1]
    top_ref[...] = res_ref[:K, :rows]
    lse_ref[...] = res_ref[K : K + 1, :rows]


def on_device(nd, nz, caption_vectors, logit_multiplier, picture_vectors):
    rows, width = caption_vectors.shape
    images = picture_vectors.shape[0]
    half = images // (2 * nd)
    nsrc = nd * nz
    vmem = pl.BlockSpec(memory_space=pltpu.VMEM)
    f32 = jnp.float32
    res = pl.pallas_call(
        functools.partial(kernel, nd, nz, (width * nd) ** (-0.5)),
        out_shape=pltpu.VMEM((LIST, LANES), f32),
        in_specs=[pl.BlockSpec(memory_space=pl.ANY)]*3,
        out_specs=vmem,
        scratch_shapes=[
            pltpu.VMEM((rows, width), jnp.bfloat16),
            pltpu.VMEM((1, rows), f32),
            pltpu.SemaphoreType.DMA((2,)),
            pltpu.VMEM((nd, width, 2 * half), jnp.bfloat16),
            pltpu.VMEM((nd, 2 * half, width), jnp.bfloat16),
            pltpu.VMEM((nz, LANES + LANES // 2, width), jnp.bfloat16),
            pltpu.VMEM((nz, half, LANES), f32),
            pltpu.VMEM((nz, max(nd - 1, 1), half + TAIL, LANES), jnp.bfloat16),
            pltpu.VMEM((nz, max(nd - 1, 1), half + TAIL, LANES), jnp.bfloat16),
            pltpu.VMEM((nz, PAY, LANES), f32),
            pltpu.VMEM((nsrc, PAY, LANES), f32),
            pltpu.SemaphoreType.DMA((nd,)),
            pltpu.SemaphoreType.DMA((nz,)),
            pltpu.SemaphoreType.DMA((nz,)),
            pltpu.SemaphoreType.DMA((nz, max(nd - 1, 1))),
            pltpu.SemaphoreType.DMA((nz, max(nd - 1, 1))),
            pltpu.SemaphoreType.DMA((nz, nd)),
            pltpu.SemaphoreType.DMA((nz, nd)),
        ],
        compiler_params=pltpu.CompilerParams(collective_id=0, has_side_effects=True),
    )(caption_vectors, logit_multiplier.reshape(1, rows), picture_vectors.T)
    lse, top = pl.pallas_call(
        split_kernel,
        out_shape=(jax.ShapeDtypeStruct((1, rows), f32), jax.ShapeDtypeStruct((K, rows), f32)),
        in_specs=[vmem],
        out_specs=(vmem, vmem),
    )(pltpu.with_memory_space_constraint(res, pltpu.VMEM))
    return lse.reshape(rows), top.T


def solution(mesh):
    placed = (P(("grp", "img", "qry"), "dim"), P(("grp", "img", "qry")), P(("grp", "img"), "dim"))
    return jax.shard_map(
        functools.partial(on_device, mesh.shape["dim"], mesh.shape["img"]),
        mesh=mesh,
        in_specs=placed,
        out_specs=(P(("grp", "img", "qry")), P(("grp", "img", "qry"), None)),
        check_vma=False,
    )
```
